32 devices in a mesh: rows: 4 (over z), bundle: 8 (over y, x, core).
Axes of the slice: x: 2, y: 2, z: 4, core: 2. Of those that a mesh axis runs over, the one named last changes fastest.
Arguments:
- raw_values: float32 [8192, 4096], P(('rows', 'bundle')), may hold values from -2100 to 2100
- bin_edges: float32 [4096, 255], P(('rows', 'bundle')), may hold values from -2100 to 2100, as said below
- feature_column: int32 [4096], replicated, may hold values from 0 to 4095, each once
- bin_offset: int32 [4096], replicated, may hold values from 0 to 63
Outputs:
- bin_codes: int32 [8192, 4096], P('rows', 'bundle')
The draws below stay inside these ranges and needn't reach their ends.
Inputs may be any that keep to these rules, and one draw needn't show every extreme that they name: Every row of bin_edges is strictly increasing. `feature_column`: each column 0 .. 4095 is named once.
All inputs are finite; a program needn't handle non-finite values.
Results may differ from the reference program's by a relative error of at most 0.0003.
Values may be sent and summed in bfloat16 or wider, within the bound.
A program may use at most 64 MiB of HBM per device.

```python
import math
import jax
import jax.numpy as jnp
from jax import lax

FEATURE_COUNT = 4096
BOUNDARY_COUNT = 255
ROWS = 8192


def feature_frame(key):
    center_key = jax.random.fold_in(key, 21)
    stretch_key = jax.random.fold_in(key, 22)
    magnitude = jax.random.uniform(center_key, (FEATURE_COUNT,), jnp.float32, 256.0, 2048.0)
    center = magnitude
    stretch = jnp.exp(jax.random.uniform(stretch_key, (FEATURE_COUNT,), jnp.float32, -0.69, 0.69))
    return (center, stretch)


def draw_raw_values(key, part):
    center, stretch = feature_frame(key)
    noise_key = jax.random.fold_in(key, 31)
    unit = jax.random.truncated_normal(noise_key, -6.0, 6.0, (ROWS, FEATURE_COUNT), jnp.float32)
    return (center[None, :] + stretch[None, :] * unit).astype(jnp.float32)


def draw_bin_edges(key, part):
    center, stretch = feature_frame(key)
    steps_key = jax.random.fold_in(key, 11)
    spike_random_key = jax.random.fold_in(key, 12)
    step_increments = jnp.exp(jax.random.uniform(steps_key, (FEATURE_COUNT, BOUNDARY_COUNT), jnp.float32, -3.0, 0.69))
    edge_positions = jax.random.randint(spike_random_key, (FEATURE_COUNT, 3), 0, BOUNDARY_COUNT)
    column_values = jnp.arange(BOUNDARY_COUNT, dtype=jnp.int32)
    spike_values = jnp.any(column_values[None, :, None] == edge_positions[:, None, :], axis=2)
    step_increments = step_increments * jnp.where(spike_values, 30.0, 1.0)
    running = jnp.cumsum(step_increments, axis=1)
    unit = -3.0 + 6.0 * running / (running[:, -1:] + 1.0)
    edges = center[:, None] + stretch[:, None] * unit
    return edges.astype(jnp.float32)


def place_ends(values, key, least, largest):
    index_at = [jax.random.randint(jax.random.fold_in(key, axis), (), 0, length) for axis, length in enumerate(values.shape)]
    widest = values.shape.index(max(values.shape))
    next_to = index_at[:widest] + [(index_at[widest] + 1) % values.shape[widest]] + index_at[widest + 1:]
    return values.at[tuple(index_at)].set(least).at[tuple(next_to)].set(largest)


def setup_inputs(seed: int = 0) -> dict:
    key_of = jax.random.split(jax.random.key(seed), 5)
    return {
        "raw_values": draw_raw_values(jax.random.fold_in(key_of[4], 71), 0),
        "bin_edges": draw_bin_edges(jax.random.fold_in(key_of[4], 71), 0),
        "feature_column": jax.random.permutation(key_of[2], FEATURE_COUNT).astype(jnp.int32),
        "bin_offset": place_ends(jax.random.randint(key_of[3], (FEATURE_COUNT,), 0, 64), jax.random.fold_in(key_of[3], 1), 0, 63).astype(jnp.int32),
    }


def count_below(values, edges):
    total = values.shape[0]
    block = math.gcd(total, 512)

    def one_block(part_rows):
        return jnp.sum(part_rows[:, :, None] > edges[None, :, :], axis=2, dtype=jnp.int32)

    blocks = values.reshape(total // block, block, values.shape[1])
    return lax.map(one_block, blocks).reshape(total, values.shape[1])


def reference(raw_values, bin_edges, feature_column, bin_offset):
    count_feat = feature_column.shape[0]
    owner_feature = jnp.zeros((count_feat,), jnp.int32).at[feature_column].set(jnp.arange(count_feat, dtype=jnp.int32))
    ordered = jnp.take(raw_values, owner_feature, axis=1)
    edges = jnp.take(bin_edges, owner_feature, axis=0)
    bins = count_below(ordered, edges)
    return bins + jnp.take(bin_offset, owner_feature)[None, :]
```

```python
import functools

import jax
import jax.numpy as jnp
from jax import lax
from jax.experimental import pallas as pl
from jax.experimental.pallas import tpu as pltpu
from jax.sharding import PartitionSpec as P

LANES = 128


def lane_gather(table, index):
    return jnp.take_along_axis(table, index, axis=1, mode="promise_in_bounds")


def table_kernel(edges_ref, offset_ref, table_ref):
    low, high = edges_ref[:, :LANES], edges_ref[:, LANES:]
    lane = lax.broadcasted_iota(jnp.int32, low.shape, 1)
    edge = jnp.zeros_like(lane)
    for level in range(7):
        width = 1 << level
        at_level = (lane >= width) & (lane < 2 * width)
        edge = jnp.where(at_level, (2 * (lane - width) + 1) * (LANES // width) - 1, edge)

    def pick(index):
        inner = index & (LANES - 1)
        return jnp.where(index < LANES, lane_gather(low, inner), lane_gather(high, inner))

    offset = jnp.broadcast_to(offset_ref[...], low.shape)
    table_ref[:, :LANES] = jnp.where(lane == 0, offset, pick(edge))
    table_ref[:, LANES:] = pick(2 * lane)


def make_tables(edges, offsets):
    count = edges.shape[0]
    return pl.pallas_call(
        table_kernel,
        out_shape=jax.ShapeDtypeStruct((count, 2 * LANES), jnp.float32),
        name="make_tables",
    )(jnp.pad(edges, ((0, 0), (0, 2 * LANES - edges.shape[1]))), offsets)


def bin_kernel(column_ref, raw_ref, table_ref, code_ref):
    features = raw_ref.shape[1]
    first = pl.program_id(0) * features
    group = 64
    for start in range(0, features, group):
        values = raw_ref[:, start : start + group].T
        tree = table_ref[start : start + group, :LANES]
        leaves = table_ref[start : start + group, LANES:]
        root = jnp.broadcast_to(tree[:, 1:2], tree.shape)
        halves = []
        for half in range(2):
            x = values[:, half * LANES : (half + 1) * LANES]
            node = jnp.where(x > root, 3, 2)
            for _ in range(6):
                node = 2 * node + jnp.where(x > lane_gather(tree, node), 1, 0)
            leaf = node - LANES
            halves.append(2 * leaf + jnp.where(x > lane_gather(leaves, leaf), 1, 0))
        offset = jnp.broadcast_to(tree[:, 0:1], tree.shape).astype(jnp.int32)
        packed = halves[0] + halves[1] * 65536 + offset * 65537
        for row in range(group):
            column = column_ref[first + start + row]
            code_ref[pl.ds(column, 1), :] = packed[row : row + 1, :]


def bin_rows(column, raw, tables):
    rows, features = raw.shape
    block = 128
    return pl.pallas_call(
        bin_kernel,
        grid_spec=pltpu.PrefetchScalarGridSpec(
            num_scalar_prefetch=1,
            grid=(features // block,),
            in_specs=[
                pl.BlockSpec((rows, block), lambda i, c: (0, i)),
                pl.BlockSpec((block, 2 * LANES), lambda i, c: (i, 0)),
            ],
            out_specs=pl.BlockSpec((features, rows // 2), lambda i, c: (0, 0)),
        ),
        out_shape=jax.ShapeDtypeStruct((features, rows // 2), jnp.int32),
        name="bin_rows",
    )(column, raw, tables)


def unpack_kernel(code_ref, out_ref):
    half = code_ref.shape[2]
    codes = code_ref[0].T
    out_ref[:half, :] = codes & 65535
    out_ref[half:, :] = codes >> 16


def unpack(codes):
    sources, columns, half = codes.shape
    return pl.pallas_call(
        unpack_kernel,
        grid=(sources,),
        in_specs=[pl.BlockSpec((1, columns, half), lambda i: (i, 0, 0))],
        out_specs=pl.BlockSpec((2 * half, columns), lambda i: (i, 0)),
        out_shape=jax.ShapeDtypeStruct((sources * 2 * half, columns), jnp.int32),
        name="unpack",
    )(codes)


def local(raw_values, bin_edges, feature_column, bin_offset):
    bundles = lax.axis_size("bundle")
    features = feature_column.shape[0]
    held = bin_edges.shape[0]
    first = (lax.axis_index("rows") * bundles + lax.axis_index("bundle")) * held
    offsets = lax.dynamic_slice_in_dim(bin_offset, first, held, 0)
    tables = make_tables(bin_edges, offsets.astype(jnp.float32)[:, None])
    tables = lax.all_gather(tables, ("rows", "bundle"), axis=0, tiled=True)
    codes = bin_rows(feature_column, raw_values, tables)
    codes = codes.reshape(bundles, features // bundles, codes.shape[1])
    codes = lax.all_to_all(codes, "bundle", split_axis=0, concat_axis=0, tiled=True)
    return unpack(codes)


def solution(mesh):
    in_specs = (P(("rows", "bundle"), None), P(("rows", "bundle"), None), P(), P())
    out_specs = P("rows", "bundle")
    return jax.shard_map(local, mesh=mesh, in_specs=in_specs, out_specs=out_specs, check_vma=False)
```

```python
import functools

import jax
import jax.numpy as jnp
from jax import lax
from jax.experimental import pallas as pl
from jax.experimental.pallas import tpu as pltpu
from jax.sharding import PartitionSpec as P

LANES = 128
MESH = pl.DeviceIdType.MESH


def lane_gather(table, index):
    return jnp.take_along_axis(table, index, axis=1, mode="promise_in_bounds")


def table_kernel(edges_ref, offset_ref, table_ref):
    low, high = edges_ref[:, :LANES], edges_ref[:, LANES:]
    lane = lax.broadcasted_iota(jnp.int32, low.shape, 1)
    edge = jnp.zeros_like(lane)
    for level in range(7):
        width = 1 << level
        at_level = (lane >= width) & (lane < 2 * width)
        edge = jnp.where(at_level, (2 * (lane - width) + 1) * (LANES // width) - 1, edge)

    def pick(index):
        inner = index & (LANES - 1)
        return jnp.where(index < LANES, lane_gather(low, inner), lane_gather(high, inner))

    offset = jnp.broadcast_to(offset_ref[...], low.shape)
    table_ref[:, :LANES] = jnp.where(lane == 0, offset, pick(edge))
    table_ref[:, LANES:] = pick(2 * lane)


def make_tables(edges, offsets):
    count = edges.shape[0]
    return pl.pallas_call(
        table_kernel,
        out_shape=jax.ShapeDtypeStruct((count, 2 * LANES), jnp.float32),
        name="make_tables",
    )(jnp.pad(edges, ((0, 0), (0, 2 * LANES - edges.shape[1]))), offsets)


def gather_kernel(table_ref, all_ref, send_sem, row_sem, side_sem, relay_sem, partner_sem):
    held = table_ref.shape[0]
    rows, bundles = lax.axis_size("rows"), lax.axis_size("bundle")
    row, bundle = lax.axis_index("rows"), lax.axis_index("bundle")
    sides = bundles // 2
    partner = bundle + 1 - 2 * lax.rem(bundle, 2)
    side = [lax.rem(bundle + 2 * step, bundles) for step in range(sides)]
    source = [lax.rem(bundle + bundles - 2 * step, bundles) for step in range(sides)]
    group = [lax.rem(row + step, rows) for step in range(rows)]
    origin = [lax.rem(row + rows - step, rows) for step in range(rows)]
    square = sides == 4
    if square:
        pair = lax.div(bundle, 2)
        across = bundle + 2 - 4 * lax.rem(pair, 2)
        along = bundle + 4 - 8 * lax.div(pair, 2)
        corner = across + 4 - 8 * lax.div(pair, 2)

    barrier = pltpu.get_barrier_semaphore()
    others = [(peer, bundle) for peer in group[1:]] + [(row, partner)]
    others += [(row, across), (row, along)] if square else [(row, peer) for peer in side[1:]]
    for peer in others:
        pl.semaphore_signal(barrier, inc=1, device_id=peer, device_id_type=MESH)
    pl.semaphore_wait(barrier, len(others))

    def at(row_index, bundle_index, start=0, size=held):
        first = (row_index * bundles + bundle_index) * held + start
        return all_ref.at[pl.ds(pl.multiple_of(first, 8), size)]

    sent = []

    def send(block, source_ref, device, arrival):
        copy = pltpu.make_async_remote_copy(
            src_ref=source_ref,
            dst_ref=block,
            send_sem=send_sem.at[len(sent)],
            recv_sem=arrival,
            device_id=device,
            device_id_type=MESH,
        )
        copy.start()
        sent.append(copy)

    def arrived(block, arrival):
        pltpu.make_async_copy(block, block, arrival).wait()

    for step in range(1, rows):
        send(at(row, bundle), table_ref, (group[step], bundle), row_sem.at[step])
    all_ref[pl.ds(pl.multiple_of((row * bundles + bundle) * held, 8), held), :] = table_ref[...]
    half = held // 2
    for step in range(rows):
        block = at(origin[step], bundle)
        if step:
            arrived(block, row_sem.at[step])
        from_ref = block if step else table_ref
        if square:
            send(block, from_ref, (row, across), side_sem.at[step, 1])
            send(block, from_ref, (row, along), side_sem.at[step, 2])
        else:
            for turn in range(1, sides):
                send(block, from_ref, (row, side[turn]), side_sem.at[step, turn])
        send(block, from_ref, (row, partner), partner_sem.at[step, 0])
    for step in range(rows):
        if square:
            block = at(origin[step], across)
            arrived(block, side_sem.at[step, 1])
            tail = at(origin[step], across, half, half)
            send(tail, tail, (row, along), relay_sem.at[step, 1])
            send(block, block, (row, partner), partner_sem.at[step, 1])
            block = at(origin[step], along)
            arrived(block, side_sem.at[step, 2])
            head = at(origin[step], along, 0, half)
            send(head, head, (row, across), relay_sem.at[step, 0])
            send(block, block, (row, partner), partner_sem.at[step, 2])
        else:
            for turn in range(1, sides):
                block = at(origin[step], source[turn])
                arrived(block, side_sem.at[step, turn])
                send(block, block, (row, partner), partner_sem.at[step, turn])
    if square:
        for step in range(rows):
            arrived(at(origin[step], corner, 0, half), relay_sem.at[step, 0])
            arrived(at(origin[step], corner, half, half), relay_sem.at[step, 1])
            block = at(origin[step], corner)
            send(block, block, (row, partner), partner_sem.at[step, 3])
    opposite = [partner] + ([across, along, corner] if square else source[1:])
    for step in range(rows):
        for turn in range(sides):
            mate = partner if turn == 0 else opposite[turn] + 1 - 2 * lax.rem(bundle, 2)
            arrived(at(origin[step], mate), partner_sem.at[step, turn])
    for copy in sent:
        copy.wait_send()


def gather_tables(tables):
    held, width = tables.shape
    rows, bundles = lax.axis_size("rows"), lax.axis_size("bundle")
    sides = bundles // 2
    sends = rows - 1 + rows * 3 * sides
    return pl.pallas_call(
        gather_kernel,
        out_shape=jax.ShapeDtypeStruct((rows * bundles * held, width), jnp.float32),
        in_specs=[pl.BlockSpec(memory_space=pltpu.VMEM)],
        out_specs=pl.BlockSpec(memory_space=pltpu.VMEM),
        scratch_shapes=[
            pltpu.SemaphoreType.DMA((sends,)),
            pltpu.SemaphoreType.DMA((rows,)),
            pltpu.SemaphoreType.DMA((rows, sides)),
            pltpu.SemaphoreType.DMA((rows, 2)),
            pltpu.SemaphoreType.DMA((rows, sides)),
        ],
        compiler_params=pltpu.CompilerParams(collective_id=0, has_side_effects=True),
        name="gather_tables",
    )(tables)


def bin_kernel(column_ref, raw_ref, table_ref, code_ref):
    features = raw_ref.shape[1]
    first = pl.program_id(0) * features
    group = 64
    for start in range(0, features, group):
        values = raw_ref[:, start : start + group].T
        tree = table_ref[start : start + group, :LANES]
        leaves = table_ref[start : start + group, LANES:]
        root = jnp.broadcast_to(tree[:, 1:2], tree.shape)
        halves = []
        for half in range(2):
            x = values[:, half * LANES : (half + 1) * LANES]
            node = jnp.where(x > root, 3, 2)
            for _ in range(6):
                node = 2 * node + jnp.where(x > lane_gather(tree, node), 1, 0)
            leaf = node - LANES
            halves.append(2 * leaf + jnp.where(x > lane_gather(leaves, leaf), 1, 0))
        offset = jnp.broadcast_to(tree[:, 0:1], tree.shape).astype(jnp.int32)
        packed = halves[0] + halves[1] * 65536 + offset * 65537
        for row in range(group):
            column = column_ref[first + start + row]
            code_ref[pl.ds(column, 1), :] = packed[row : row + 1, :]


def bin_rows(column, raw, tables):
    rows, features = raw.shape
    block = 128
    return pl.pallas_call(
        bin_kernel,
        grid_spec=pltpu.PrefetchScalarGridSpec(
            num_scalar_prefetch=1,
            grid=(features // block,),
            in_specs=[
                pl.BlockSpec((rows, block), lambda i, c: (0, i)),
                pl.BlockSpec((block, 2 * LANES), lambda i, c: (i, 0)),
            ],
            out_specs=pl.BlockSpec((features, rows // 2), lambda i, c: (0, 0)),
        ),
        out_shape=jax.ShapeDtypeStruct((features, rows // 2), jnp.int32),
        name="bin_rows",
    )(column, raw, tables)


def unpack_kernel(code_ref, out_ref):
    half = code_ref.shape[2]
    codes = code_ref[0].T
    out_ref[:half, :] = codes & 65535
    out_ref[half:, :] = codes >> 16


def unpack(codes):
    sources, columns, half = codes.shape
    return pl.pallas_call(
        unpack_kernel,
        grid=(sources,),
        in_specs=[pl.BlockSpec((1, columns, half), lambda i: (i, 0, 0))],
        out_specs=pl.BlockSpec((2 * half, columns), lambda i: (i, 0)),
        out_shape=jax.ShapeDtypeStruct((sources * 2 * half, columns), jnp.int32),
        name="unpack",
    )(codes)


def local(raw_values, bin_edges, feature_column, bin_offset):
    bundles = lax.axis_size("bundle")
    features = feature_column.shape[0]
    held = bin_edges.shape[0]
    first = (lax.axis_index("rows") * bundles + lax.axis_index("bundle")) * held
    offsets = lax.dynamic_slice_in_dim(bin_offset, first, held, 0)
    tables = make_tables(bin_edges, offsets.astype(jnp.float32)[:, None])
    tables = gather_tables(tables)
    codes = bin_rows(feature_column, raw_values, tables)
    codes = codes.reshape(bundles, features // bundles, codes.shape[1])
    codes = lax.all_to_all(codes, "bundle", split_axis=0, concat_axis=0, tiled=True)
    return unpack(codes)


def solution(mesh):
    in_specs = (P(("rows", "bundle"), None), P(("rows", "bundle"), None), P(), P())
    out_specs = P("rows", "bundle")
    return jax.shard_map(local, mesh=mesh, in_specs=in_specs, out_specs=out_specs, check_vma=False)
```

```python
import functools

import jax
import jax.numpy as jnp
from jax import lax
from jax.experimental import pallas as pl
from jax.experimental.pallas import tpu as pltpu
from jax.sharding import PartitionSpec as P

LANES = 128
BLOCK = 128
MESH = pl.DeviceIdType.MESH


def lane_gather(table, index):
    return lax.gather(
        table,
        index[:, :, None],
        lax.GatherDimensionNumbers(
            offset_dims=(),
            collapsed_slice_dims=(1,),
            start_index_map=(1,),
            operand_batching_dims=(0,),
            start_indices_batching_dims=(0,),
        ),
        slice_sizes=(1, 1),
        mode=lax.GatherScatterMode.PROMISE_IN_BOUNDS,
    )


def table_kernel(edges_ref, offset_ref, table_ref):
    edges = edges_ref[...]
    tail = jnp.broadcast_to(offset_ref[...].astype(jnp.float32), (edges.shape[0], 2 * LANES - edges.shape[1]))
    low = edges[:, :LANES]
    high = jnp.concatenate([edges[:, LANES:], tail], axis=1)
    lane = lax.broadcasted_iota(jnp.int32, low.shape, 1)
    for start in range(2):
        index = 2 * lane + 1 - start
        inner = index & (LANES - 1)
        picked = jnp.where(index < LANES, lane_gather(low, inner), lane_gather(high, inner))
        table_ref[:, start * LANES : (start + 1) * LANES] = picked


def make_tables(edges, offsets):
    count = edges.shape[0]
    return pl.pallas_call(
        table_kernel,
        out_shape=jax.ShapeDtypeStruct((count, 2 * LANES), jnp.float32),
        name="make_tables",
    )(edges, offsets)


def gather_kernel(table_ref, all_ref, send_sem, row_sem, side_sem, relay_sem, partner_sem):
    held = table_ref.shape[0]
    rows, bundles = lax.axis_size("rows"), lax.axis_size("bundle")
    row, bundle = lax.axis_index("rows"), lax.axis_index("bundle")
    sides = bundles // 2
    partner = bundle + 1 - 2 * lax.rem(bundle, 2)
    side = [lax.rem(bundle + 2 * step, bundles) for step in range(sides)]
    source = [lax.rem(bundle + bundles - 2 * step, bundles) for step in range(sides)]
    group = [lax.rem(row + step, rows) for step in range(rows)]
    origin = [lax.rem(row + rows - step, rows) for step in range(rows)]
    square = sides == 4
    if square:
        pair = lax.div(bundle, 2)
        across = bundle + 2 - 4 * lax.rem(pair, 2)
        along = bundle + 4 - 8 * lax.div(pair, 2)
        corner = across + 4 - 8 * lax.div(pair, 2)

    barrier = pltpu.get_barrier_semaphore()
    others = [(peer, bundle) for peer in group[1:]] + [(row, partner)]
    others += [(row, across), (row, along)] if square else [(row, peer) for peer in side[1:]]
    for peer in others:
        pl.semaphore_signal(barrier, inc=1, device_id=peer, device_id_type=MESH)
    pl.semaphore_wait(barrier, len(others))

    def at(row_index, bundle_index, start=0, size=held):
        first = (row_index * bundles + bundle_index) * held + start
        return all_ref.at[pl.ds(pl.multiple_of(first, 8), size)]

    sent = []

    def send(block, source_ref, device, arrival):
        copy = pltpu.make_async_remote_copy(
            src_ref=source_ref,
            dst_ref=block,
            send_sem=send_sem.at[len(sent)],
            recv_sem=arrival,
            device_id=device,
            device_id_type=MESH,
        )
        copy.start()
        sent.append(copy)

    def arrived(block, arrival):
        pltpu.make_async_copy(block, block, arrival).wait()

    for step in range(1, rows):
        send(at(row, bundle), table_ref, (group[step], bundle), row_sem.at[step])
    all_ref[pl.ds(pl.multiple_of((row * bundles + bundle) * held, 8), held), :] = table_ref[...]
    half = held // 2
    for step in range(rows):
        block = at(origin[step], bundle)
        if step:
            arrived(block, row_sem.at[step])
        from_ref = block if step else table_ref
        if square:
            send(block, from_ref, (row, across), side_sem.at[step, 1])
            send(block, from_ref, (row, along), side_sem.at[step, 2])
        else:
            for turn in range(1, sides):
                send(block, from_ref, (row, side[turn]), side_sem.at[step, turn])
        send(block, from_ref, (row, partner), partner_sem.at[step, 0])
    for step in range(rows):
        if square:
            block = at(origin[step], across)
            arrived(block, side_sem.at[step, 1])
            tail = at(origin[step], across, half, half)
            send(tail, tail, (row, along), relay_sem.at[step, 1])
            send(block, block, (row, partner), partner_sem.at[step, 1])
            block = at(origin[step], along)
            arrived(block, side_sem.at[step, 2])
            head = at(origin[step], along, 0, half)
            send(head, head, (row, across), relay_sem.at[step, 0])
            send(block, block, (row, partner), partner_sem.at[step, 2])
        else:
            for turn in range(1, sides):
                block = at(origin[step], source[turn])
                arrived(block, side_sem.at[step, turn])
                send(block, block, (row, partner), partner_sem.at[step, turn])
    if square:
        for step in range(rows):
            arrived(at(origin[step], corner, 0, half), relay_sem.at[step, 0])
            arrived(at(origin[step], corner, half, half), relay_sem.at[step, 1])
            block = at(origin[step], corner)
            send(block, block, (row, partner), partner_sem.at[step, 3])
    opposite = [partner] + ([across, along, corner] if square else source[1:])
    for step in range(rows):
        for turn in range(sides):
            mate = partner if turn == 0 else opposite[turn] + 1 - 2 * lax.rem(bundle, 2)
            arrived(at(origin[step], mate), partner_sem.at[step, turn])
    for copy in sent:
        copy.wait_send()


def gather_tables(tables):
    held, width = tables.shape
    rows, bundles = lax.axis_size("rows"), lax.axis_size("bundle")
    sides = bundles // 2
    sends = rows - 1 + rows * 3 * sides
    return pl.pallas_call(
        gather_kernel,
        out_shape=jax.ShapeDtypeStruct((rows * bundles * held, width), jnp.float32),
        in_specs=[pl.BlockSpec(memory_space=pltpu.VMEM)],
        out_specs=pl.BlockSpec(memory_space=pltpu.VMEM),
        scratch_shapes=[
            pltpu.SemaphoreType.DMA((sends,)),
            pltpu.SemaphoreType.DMA((rows,)),
            pltpu.SemaphoreType.DMA((rows, sides)),
            pltpu.SemaphoreType.DMA((rows, 2)),
            pltpu.SemaphoreType.DMA((rows, sides)),
        ],
        compiler_params=pltpu.CompilerParams(collective_id=0, has_side_effects=True),
        name="gather_tables",
    )(tables)


def bin_codes_of(values, table):
    odd, even = table[:, :LANES], table[:, LANES:]
    middle = LANES // 2 - 1
    root = jnp.broadcast_to(odd[:, middle : middle + 1], odd.shape)
    halves = []
    for half in range(2):
        x = values[:, half * LANES : (half + 1) * LANES]
        step = LANES // 4
        at = jnp.where(x > root, middle + step, middle - step)
        while step > 1:
            step //= 2
            at = at + jnp.where(x > lane_gather(odd, at), step, -step)
        at = at + jnp.where(x > lane_gather(odd, at), 1, 0)
        halves.append(at + at + jnp.where(x > lane_gather(even, at), 1, 0))
    offset = jnp.broadcast_to(odd[:, LANES - 1 :], odd.shape).astype(jnp.int32)
    low, high = halves[0] + offset, halves[1] + offset
    return low | (high << 16)


def bin_kernel(column_ref, raw_ref, table_ref, code_ref):
    features = raw_ref.shape[1]
    first = pl.program_id(0) * features
    packed = bin_codes_of(raw_ref[...].T, table_ref[...])
    for row in range(features):
        code_ref[pl.ds(column_ref[first + row], 1), :] = packed[row : row + 1, :]


def bin_rows(column, raw, tables):
    rows, features = raw.shape
    block = BLOCK
    return pl.pallas_call(
        bin_kernel,
        grid_spec=pltpu.PrefetchScalarGridSpec(
            num_scalar_prefetch=1,
            grid=(features // block,),
            in_specs=[
                pl.BlockSpec((rows, block), lambda i, c: (0, i)),
                pl.BlockSpec((block, 2 * LANES), lambda i, c: (i, 0)),
            ],
            out_specs=pl.BlockSpec((features, rows // 2), lambda i, c: (0, 0)),
        ),
        out_shape=jax.ShapeDtypeStruct((features, rows // 2), jnp.int32),
        name="bin_rows",
    )(column, raw, tables)


def unpack_kernel(code_ref, out_ref):
    half = code_ref.shape[2]
    codes = code_ref[0].T
    out_ref[:half, :] = codes & 65535
    out_ref[half:, :] = codes >> 16


def unpack(codes):
    sources, columns, half = codes.shape
    return pl.pallas_call(
        unpack_kernel,
        grid=(sources,),
        in_specs=[pl.BlockSpec((1, columns, half), lambda i: (i, 0, 0))],
        out_specs=pl.BlockSpec((2 * half, columns), lambda i: (i, 0)),
        out_shape=jax.ShapeDtypeStruct((sources * 2 * half, columns), jnp.int32),
        name="unpack",
    )(codes)


def local(raw_values, bin_edges, feature_column, bin_offset):
    bundles = lax.axis_size("bundle")
    features = feature_column.shape[0]
    held = bin_edges.shape[0]
    first = (lax.axis_index("rows") * bundles + lax.axis_index("bundle")) * held
    offsets = lax.dynamic_slice_in_dim(bin_offset, first, held, 0)
    tables = make_tables(bin_edges, offsets[:, None])
    tables = gather_tables(tables)
    codes = bin_rows(feature_column, raw_values, tables)
    codes = codes.reshape(bundles, features // bundles, codes.shape[1])
    codes = lax.all_to_all(codes, "bundle", split_axis=0, concat_axis=0, tiled=True)
    return unpack(codes)


def solution(mesh):
    in_specs = (P(("rows", "bundle"), None), P(("rows", "bundle"), None), P(), P())
    out_specs = P("rows", "bundle")
    return jax.shard_map(local, mesh=mesh, in_specs=in_specs, out_specs=out_specs, check_vma=False)
```

```python
import functools

import jax
import jax.numpy as jnp
from jax import lax
from jax.experimental import pallas as pl
from jax.experimental.pallas import tpu as pltpu
from jax.sharding import PartitionSpec as P

LANES = 128
BLOCK = 128
MESH = pl.DeviceIdType.MESH


def lane_gather(table, index):
    return lax.gather(
        table,
        index[:, :, None],
        lax.GatherDimensionNumbers(
            offset_dims=(),
            collapsed_slice_dims=(1,),
            start_index_map=(1,),
            operand_batching_dims=(0,),
            start_indices_batching_dims=(0,),
        ),
        slice_sizes=(1, 1),
        mode=lax.GatherScatterMode.PROMISE_IN_BOUNDS,
    )


def table_kernel(edges_ref, offset_ref, table_ref):
    edges = edges_ref[...]
    tail = jnp.broadcast_to(offset_ref[...].astype(jnp.float32), (edges.shape[0], 2 * LANES - edges.shape[1]))
    low = edges[:, :LANES]
    high = jnp.concatenate([edges[:, LANES:], tail], axis=1)
    lane = lax.broadcasted_iota(jnp.int32, low.shape, 1)
    for start in range(2):
        index = 2 * lane + 1 - start
        inner = index & (LANES - 1)
        picked = jnp.where(index < LANES, lane_gather(low, inner), lane_gather(high, inner))
        table_ref[:, start * LANES : (start + 1) * LANES] = picked


def make_tables(edges, offsets):
    count = edges.shape[0]
    return pl.pallas_call(
        table_kernel,
        out_shape=jax.ShapeDtypeStruct((count, 2 * LANES), jnp.float32),
        name="make_tables",
    )(edges, offsets)


def bin_codes_of(values, table):
    odd, even = table[:, :LANES], table[:, LANES:]
    middle = LANES // 2 - 1
    root = jnp.broadcast_to(odd[:, middle : middle + 1], odd.shape)
    halves = []
    for half in range(2):
        x = values[:, half * LANES : (half + 1) * LANES]
        step = LANES // 4
        at = jnp.where(x > root, middle + step, middle - step)
        while step > 1:
            step //= 2
            at = at + jnp.where(x > lane_gather(odd, at), step, -step)
        at = at + jnp.where(x > lane_gather(odd, at), 1, 0)
        halves.append(at + at + jnp.where(x > lane_gather(even, at), 1, 0))
    offset = jnp.broadcast_to(odd[:, LANES - 1 :], odd.shape).astype(jnp.int32)
    low, high = halves[0] + offset, halves[1] + offset
    return low | (high << 16)


def bin_kernel(
    table_ref, raw_hbm, code_ref, all_ref, raw_ref, values_ref, raw_sem, send_sem, row_sem, side_sem, relay_sem, partner_sem
):
    held = table_ref.shape[0]
    rows, bundles = lax.axis_size("rows"), lax.axis_size("bundle")
    row, bundle = lax.axis_index("rows"), lax.axis_index("bundle")
    sides = bundles // 2
    flip = 1 - 2 * lax.rem(bundle, 2)
    partner = bundle + flip
    group = [lax.rem(row + step, rows) for step in range(rows)]
    origin = [lax.rem(row + rows - step, rows) for step in range(rows)]
    square = sides == 4
    if square:
        pair = lax.div(bundle, 2)
        across = bundle + 2 - 4 * lax.rem(pair, 2)
        along = bundle + 4 - 8 * lax.div(pair, 2)
        corner = across + 4 - 8 * lax.div(pair, 2)
        target = [bundle, across, along]
        source = [bundle, across, along, corner]
    else:
        target = [lax.rem(bundle + 2 * step, bundles) for step in range(sides)]
        source = [lax.rem(bundle + bundles - 2 * step, bundles) for step in range(sides)]
    near = len(target)

    fetch = pltpu.make_async_copy(raw_hbm, raw_ref, raw_sem)
    fetch.start()
    barrier = pltpu.get_barrier_semaphore()
    others = [(peer, bundle) for peer in group[1:]] + [(row, peer) for peer in target[1:]] + [(row, partner)]
    for peer in others:
        pl.semaphore_signal(barrier, inc=1, device_id=peer, device_id_type=MESH)
    pl.semaphore_wait(barrier, len(others))

    def place(row_index, bundle_index):
        return (row_index * bundles + bundle_index) * held

    def at(row_index, bundle_index, start=0, size=held):
        first = place(row_index, bundle_index) + start
        return all_ref.at[pl.ds(pl.multiple_of(first, 8), size)]

    sent = []

    def send(block, source_ref, device, arrival):
        copy = pltpu.make_async_remote_copy(
            src_ref=source_ref,
            dst_ref=block,
            send_sem=send_sem.at[len(sent)],
            recv_sem=arrival,
            device_id=device,
            device_id_type=MESH,
        )
        copy.start()
        sent.append(copy)

    def arrived(block, arrival):
        pltpu.make_async_copy(block, block, arrival).wait()

    def use(blocks):
        firsts = [place(*block) for block in blocks]

        def body(index, carry):
            first = firsts[0]
            for other in range(1, len(firsts)):
                first = jnp.where(index == other, firsts[other], first)
            span = pl.ds(pl.multiple_of(first, 8), held)
            code_ref[span, :] = bin_codes_of(values_ref[span, :], all_ref[span, :])
            return carry

        lax.fori_loop(0, len(firsts), body, 0)

    half = held // 2
    for step in range(1, rows):
        send(at(row, bundle), table_ref, (group[step], bundle), row_sem.at[step])
    for stage in range(rows + 3):
        ready = []
        if stage < rows:
            block = at(origin[stage], bundle)
            if stage:
                arrived(block, row_sem.at[stage])
            from_ref = block if stage else table_ref
            for turn in range(1, near):
                send(block, from_ref, (row, target[turn]), side_sem.at[stage, turn])
            send(block, from_ref, (row, partner), partner_sem.at[stage, 0])
            ready.append((origin[stage], bundle))
        if stage == 0:
            all_ref[pl.ds(pl.multiple_of(place(row, bundle), 8), held), :] = table_ref[...]
            fetch.wait()

            def turn_over(index, carry):
                span = pl.ds(pl.multiple_of(index * LANES, LANES), LANES)
                values_ref[span, :] = raw_ref[:, span].T
                return carry

            lax.fori_loop(0, raw_ref.shape[1] // LANES, turn_over, 0)
        step = stage - 1
        if 0 <= step < rows:
            for turn in range(1, near):
                block = at(origin[step], source[turn])
                arrived(block, side_sem.at[step, turn])
                if square:
                    start = half * (2 - turn)
                    part = at(origin[step], source[turn], start, half)
                    send(part, part, (row, target[3 - turn]), relay_sem.at[step, 2 - turn])
                send(block, block, (row, partner), partner_sem.at[step, turn])
                ready.append((origin[step], source[turn]))
            arrived(at(origin[step], partner), partner_sem.at[step, 0])
            ready.append((origin[step], partner))
        step = stage - 2
        if 0 <= step < rows:
            if square:
                arrived(at(origin[step], corner, 0, half), relay_sem.at[step, 0])
                arrived(at(origin[step], corner, half, half), relay_sem.at[step, 1])
                block = at(origin[step], corner)
                send(block, block, (row, partner), partner_sem.at[step, 3])
                ready.append((origin[step], corner))
            for turn in range(1, near):
                arrived(at(origin[step], source[turn] + flip), partner_sem.at[step, turn])
                ready.append((origin[step], source[turn] + flip))
        step = stage - 3
        if 0 <= step < rows and square:
            arrived(at(origin[step], corner + flip), partner_sem.at[step, 3])
            ready.append((origin[step], corner + flip))
        if ready:
            use(ready)
    for copy in sent:
        copy.wait_send()


def bin_rows(tables, raw):
    held, width = tables.shape
    count, features = raw.shape
    rows, bundles = lax.axis_size("rows"), lax.axis_size("bundle")
    sides = bundles // 2
    sends = rows - 1 + rows * 3 * sides
    return pl.pallas_call(
        bin_kernel,
        out_shape=jax.ShapeDtypeStruct((features, count // 2), jnp.int32),
        in_specs=[pl.BlockSpec(memory_space=pltpu.VMEM), pl.BlockSpec(memory_space=pl.ANY)],
        out_specs=pl.BlockSpec(memory_space=pltpu.VMEM),
        scratch_shapes=[
            pltpu.VMEM((features, width), jnp.float32),
            pltpu.VMEM((count, features), jnp.float32),
            pltpu.VMEM((features, count), jnp.float32),
            pltpu.SemaphoreType.DMA,
            pltpu.SemaphoreType.DMA((sends,)),
            pltpu.SemaphoreType.DMA((rows,)),
            pltpu.SemaphoreType.DMA((rows, sides)),
            pltpu.SemaphoreType.DMA((rows, 2)),
            pltpu.SemaphoreType.DMA((rows, sides)),
        ],
        compiler_params=pltpu.CompilerParams(collective_id=0, has_side_effects=True),
        name="bin_rows",
    )(tables, raw)


def order_kernel(column_ref, code_ref, out_ref):
    features = code_ref.shape[0]
    first = pl.program_id(0) * features
    for row in range(features):
        out_ref[pl.ds(column_ref[first + row], 1), :] = code_ref[row : row + 1, :]


def order_columns(column, codes):
    features, width = codes.shape
    block = BLOCK
    return pl.pallas_call(
        order_kernel,
        grid_spec=pltpu.PrefetchScalarGridSpec(
            num_scalar_prefetch=1,
            grid=(features // block,),
            in_specs=[pl.BlockSpec((block, width), lambda i, c: (i, 0))],
            out_specs=pl.BlockSpec((features, width), lambda i, c: (0, 0)),
        ),
        out_shape=jax.ShapeDtypeStruct((features, width), jnp.int32),
        name="order_columns",
    )(column, codes)


def unpack_kernel(code_ref, out_ref):
    half = code_ref.shape[2]
    codes = code_ref[0].T
    out_ref[:half, :] = codes & 65535
    out_ref[half:, :] = codes >> 16


def unpack(codes):
    sources, columns, half = codes.shape
    return pl.pallas_call(
        unpack_kernel,
        grid=(sources,),
        in_specs=[pl.BlockSpec((1, columns, half), lambda i: (i, 0, 0))],
        out_specs=pl.BlockSpec((2 * half, columns), lambda i: (i, 0)),
        out_shape=jax.ShapeDtypeStruct((sources * 2 * half, columns), jnp.int32),
        name="unpack",
    )(codes)


def local(raw_values, bin_edges, feature_column, bin_offset):
    bundles = lax.axis_size("bundle")
    features = feature_column.shape[0]
    held = bin_edges.shape[0]
    first = (lax.axis_index("rows") * bundles + lax.axis_index("bundle")) * held
    offsets = lax.dynamic_slice_in_dim(bin_offset, first, held, 0)
    tables = make_tables(bin_edges, offsets[:, None])
    codes = order_columns(feature_column, bin_rows(tables, raw_values))
    codes = codes.reshape(bundles, features // bundles, codes.shape[1])
    codes = lax.all_to_all(codes, "bundle", split_axis=0, concat_axis=0, tiled=True)
    return unpack(codes)


def solution(mesh):
    in_specs = (P(("rows", "bundle"), None), P(("rows", "bundle"), None), P(), P())
    out_specs = P("rows", "bundle")
    return jax.shard_map(local, mesh=mesh, in_specs=in_specs, out_specs=out_specs, check_vma=False)
```

```python
import functools

import jax
import jax.numpy as jnp
from jax import lax
from jax.experimental import pallas as pl
from jax.experimental.pallas import tpu as pltpu
from jax.sharding import PartitionSpec as P

LANES = 128
BLOCK = 128
MESH = pl.DeviceIdType.MESH


def lane_gather(table, index):
    return lax.gather(
        table,
        index[:, :, None],
        lax.GatherDimensionNumbers(
            offset_dims=(),
            collapsed_slice_dims=(1,),
            start_index_map=(1,),
            operand_batching_dims=(0,),
            start_indices_batching_dims=(0,),
        ),
        slice_sizes=(1, 1),
        mode=lax.GatherScatterMode.PROMISE_IN_BOUNDS,
    )


def table_kernel(edges_ref, offset_ref, table_ref):
    edges = edges_ref[...]
    tail = jnp.broadcast_to(offset_ref[...].astype(jnp.float32), (edges.shape[0], 2 * LANES - edges.shape[1]))
    low = edges[:, :LANES]
    high = jnp.concatenate([edges[:, LANES:], tail], axis=1)
    lane = lax.broadcasted_iota(jnp.int32, low.shape, 1)
    for start in range(2):
        index = 2 * lane + 1 - start
        inner = index & (LANES - 1)
        picked = jnp.where(index < LANES, lane_gather(low, inner), lane_gather(high, inner))
        table_ref[:, start * LANES : (start + 1) * LANES] = picked


def make_tables(edges, offsets):
    count = edges.shape[0]
    return pl.pallas_call(
        table_kernel,
        out_shape=jax.ShapeDtypeStruct((count, 2 * LANES), jnp.float32),
        name="make_tables",
    )(edges, offsets)


def bin_codes_of(values, table):
    odd, even = table[:, :LANES], table[:, LANES:]
    middle = LANES // 2 - 1
    root = jnp.broadcast_to(odd[:, middle : middle + 1], odd.shape)
    halves = []
    for half in range(2):
        x = values[:, half * LANES : (half + 1) * LANES]
        step = LANES // 4
        at = jnp.where(x > root, middle + step, middle - step)
        while step > 1:
            step //= 2
            at = at + jnp.where(x > lane_gather(odd, at), step, -step)
        at = at + jnp.where(x > lane_gather(odd, at), 1, 0)
        halves.append(at + at + jnp.where(x > lane_gather(even, at), 1, 0))
    offset = jnp.broadcast_to(odd[:, LANES - 1 :], odd.shape).astype(jnp.int32)
    low, high = halves[0] + offset, halves[1] + offset
    return low | (high << 16)


def bin_kernel(
    table_ref, raw_hbm, code_ref, all_ref, raw_ref, values_ref, raw_sem, send_sem, row_sem, side_sem, relay_sem, partner_sem
):
    held = table_ref.shape[0]
    rows, bundles = lax.axis_size("rows"), lax.axis_size("bundle")
    row, bundle = lax.axis_index("rows"), lax.axis_index("bundle")
    sides = bundles // 2
    flip = 1 - 2 * lax.rem(bundle, 2)
    partner = bundle + flip
    group = [lax.rem(row + step, rows) for step in range(rows)]
    origin = [lax.rem(row + rows - step, rows) for step in range(rows)]
    square = sides == 4
    if square:
        pair = lax.div(bundle, 2)
        across = bundle + 2 - 4 * lax.rem(pair, 2)
        along = bundle + 4 - 8 * lax.div(pair, 2)
        corner = across + 4 - 8 * lax.div(pair, 2)
        target = [bundle, across, along]
        source = [bundle, across, along, corner]
    else:
        target = [lax.rem(bundle + 2 * step, bundles) for step in range(sides)]
        source = [lax.rem(bundle + bundles - 2 * step, bundles) for step in range(sides)]
    near = len(target)

    fetch = pltpu.make_async_copy(raw_hbm, raw_ref, raw_sem)
    fetch.start()
    barrier = pltpu.get_barrier_semaphore()
    others = [(peer, bundle) for peer in group[1:]] + [(row, peer) for peer in target[1:]] + [(row, partner)]
    for peer in others:
        pl.semaphore_signal(barrier, inc=1, device_id=peer, device_id_type=MESH)
    pl.semaphore_wait(barrier, len(others))

    def place(row_index, bundle_index):
        return (row_index * bundles + bundle_index) * held

    def at(row_index, bundle_index, start=0, size=held):
        first = place(row_index, bundle_index) + start
        return all_ref.at[pl.ds(pl.multiple_of(first, 8), size)]

    sent = []

    def send(block, source_ref, device, arrival):
        copy = pltpu.make_async_remote_copy(
            src_ref=source_ref,
            dst_ref=block,
            send_sem=send_sem.at[len(sent)],
            recv_sem=arrival,
            device_id=device,
            device_id_type=MESH,
        )
        copy.start()
        sent.append(copy)

    def arrived(block, arrival):
        pltpu.make_async_copy(block, block, arrival).wait()

    def use(blocks):
        firsts = [place(*block) for block in blocks]

        def body(index, carry):
            first = firsts[0]
            for other in range(1, len(firsts)):
                first = jnp.where(index == other, firsts[other], first)
            span = pl.ds(pl.multiple_of(first, 8), held)
            code_ref[span, :] = bin_codes_of(values_ref[span, :], all_ref[span, :])
            return carry

        lax.fori_loop(0, len(firsts), body, 0)

    half = held // 2
    for step in range(1, rows):
        send(at(row, bundle), table_ref, (group[step], bundle), row_sem.at[step])
    for stage in range(rows + 3):
        ready = []
        if stage < rows:
            block = at(origin[stage], bundle)
            if stage:
                arrived(block, row_sem.at[stage])
            from_ref = block if stage else table_ref
            for turn in range(1, near):
                send(block, from_ref, (row, target[turn]), side_sem.at[stage, turn])
            send(block, from_ref, (row, partner), partner_sem.at[stage, 0])
            ready.append((origin[stage], bundle))
        if stage == 0:
            all_ref[pl.ds(pl.multiple_of(place(row, bundle), 8), held), :] = table_ref[...]
            fetch.wait()

            def turn_over(index, carry):
                span = pl.ds(pl.multiple_of(index * LANES, LANES), LANES)
                values_ref[span, :] = raw_ref[:, span].T
                return carry

            lax.fori_loop(0, raw_ref.shape[1] // LANES, turn_over, 0)
        step = stage - 1
        if 0 <= step < rows:
            for turn in range(1, near):
                block = at(origin[step], source[turn])
                arrived(block, side_sem.at[step, turn])
                if square:
                    start = half * (2 - turn)
                    part = at(origin[step], source[turn], start, half)
                    send(part, part, (row, target[3 - turn]), relay_sem.at[step, 2 - turn])
                send(block, block, (row, partner), partner_sem.at[step, turn])
                ready.append((origin[step], source[turn]))
            arrived(at(origin[step], partner), partner_sem.at[step, 0])
            ready.append((origin[step], partner))
        step = stage - 2
        if 0 <= step < rows:
            if square:
                arrived(at(origin[step], corner, 0, half), relay_sem.at[step, 0])
                arrived(at(origin[step], corner, half, half), relay_sem.at[step, 1])
                block = at(origin[step], corner)
                send(block, block, (row, partner), partner_sem.at[step, 3])
                ready.append((origin[step], corner))
            for turn in range(1, near):
                arrived(at(origin[step], source[turn] + flip), partner_sem.at[step, turn])
                ready.append((origin[step], source[turn] + flip))
        step = stage - 3
        if 0 <= step < rows and square:
            arrived(at(origin[step], corner + flip), partner_sem.at[step, 3])
            ready.append((origin[step], corner + flip))
        if ready:
            use(ready)
    for copy in sent:
        copy.wait_send()


def bin_rows(tables, raw):
    held, width = tables.shape
    count, features = raw.shape
    rows, bundles = lax.axis_size("rows"), lax.axis_size("bundle")
    sides = bundles // 2
    sends = rows - 1 + rows * 3 * sides
    return pl.pallas_call(
        bin_kernel,
        out_shape=jax.ShapeDtypeStruct((features, count // 2), jnp.int32),
        in_specs=[pl.BlockSpec(memory_space=pltpu.VMEM), pl.BlockSpec(memory_space=pl.ANY)],
        out_specs=pl.BlockSpec(memory_space=pltpu.VMEM),
        scratch_shapes=[
            pltpu.VMEM((features, width), jnp.float32),
            pltpu.VMEM((count, features), jnp.float32),
            pltpu.VMEM((features, count), jnp.float32),
            pltpu.SemaphoreType.DMA,
            pltpu.SemaphoreType.DMA((sends,)),
            pltpu.SemaphoreType.DMA((rows,)),
            pltpu.SemaphoreType.DMA((rows, sides)),
            pltpu.SemaphoreType.DMA((rows, 2)),
            pltpu.SemaphoreType.DMA((rows, sides)),
        ],
        compiler_params=pltpu.CompilerParams(collective_id=0, has_side_effects=True),
        name="bin_rows",
    )(tables, raw)


def order_kernel(column_ref, code_ref, out_ref):
    def body(index, carry):
        first = pl.multiple_of(index * BLOCK, BLOCK)
        codes = code_ref[pl.ds(first, BLOCK), :]
        for row in range(BLOCK):
            out_ref[pl.ds(column_ref[first + row], 1), :] = codes[row : row + 1, :]
        return carry

    lax.fori_loop(0, code_ref.shape[0] // BLOCK, body, 0)


def order_columns(column, codes):
    return pl.pallas_call(
        order_kernel,
        out_shape=jax.ShapeDtypeStruct(codes.shape, jnp.int32),
        in_specs=[pl.BlockSpec(memory_space=pltpu.SMEM), pl.BlockSpec(memory_space=pltpu.VMEM)],
        out_specs=pl.BlockSpec(memory_space=pltpu.VMEM),
        name="order_columns",
    )(column, codes)


def exchange_kernel(code_ref, out_ref, own_ref, own_sem, send_sem, arrive_sem):
    bundles = lax.axis_size("bundle")
    row, bundle = lax.axis_index("rows"), lax.axis_index("bundle")
    keep = pltpu.make_async_copy(code_ref.at[bundle], own_ref, own_sem)
    keep.start()
    barrier = pltpu.get_barrier_semaphore()
    peers = [lax.rem(bundle + step, bundles) for step in range(bundles)]
    for peer in peers[1:]:
        pl.semaphore_signal(barrier, inc=1, device_id=(row, peer), device_id_type=MESH)
    pl.semaphore_wait(barrier, bundles - 1)
    sent = []
    for step in range(1, bundles):
        copy = pltpu.make_async_remote_copy(
            src_ref=code_ref.at[peers[step]],
            dst_ref=out_ref.at[bundle],
            send_sem=send_sem.at[step],
            recv_sem=arrive_sem.at[step],
            device_id=(row, peers[step]),
            device_id_type=MESH,
        )
        copy.start()
        sent.append(copy)
    keep.wait()
    keep = pltpu.make_async_copy(own_ref, out_ref.at[bundle], own_sem)
    keep.start()
    for step in range(1, bundles):
        block = out_ref.at[lax.rem(bundle + bundles - step, bundles)]
        pltpu.make_async_copy(block, block, arrive_sem.at[step]).wait()
    for copy in sent:
        copy.wait_send()
    keep.wait()


def exchange(codes):
    bundles, columns, width = codes.shape
    return pl.pallas_call(
        exchange_kernel,
        out_shape=jax.ShapeDtypeStruct(codes.shape, jnp.int32),
        in_specs=[pl.BlockSpec(memory_space=pl.ANY)],
        out_specs=pl.BlockSpec(memory_space=pl.ANY),
        scratch_shapes=[
            pltpu.VMEM((columns, width), jnp.int32),
            pltpu.SemaphoreType.DMA,
            pltpu.SemaphoreType.DMA((bundles,)),
            pltpu.SemaphoreType.DMA((bundles,)),
        ],
        compiler_params=pltpu.CompilerParams(collective_id=1, has_side_effects=True),
        name="exchange",
    )(codes)


def unpack_kernel(code_ref, out_ref):
    half = code_ref.shape[2]
    codes = code_ref[0].T
    out_ref[:half, :] = codes & 65535
    out_ref[half:, :] = codes >> 16


def unpack(codes):
    sources, columns, half = codes.shape
    return pl.pallas_call(
        unpack_kernel,
        grid=(sources,),
        in_specs=[pl.BlockSpec((1, columns, half), lambda i: (i, 0, 0))],
        out_specs=pl.BlockSpec((2 * half, columns), lambda i: (i, 0)),
        out_shape=jax.ShapeDtypeStruct((sources * 2 * half, columns), jnp.int32),
        name="unpack",
    )(codes)


def local(raw_values, bin_edges, feature_column, bin_offset):
    bundles = lax.axis_size("bundle")
    features = feature_column.shape[0]
    held = bin_edges.shape[0]
    first = (lax.axis_index("rows") * bundles + lax.axis_index("bundle")) * held
    offsets = lax.dynamic_slice_in_dim(bin_offset, first, held, 0)
    tables = make_tables(bin_edges, offsets[:, None])
    codes = order_columns(feature_column, bin_rows(tables, raw_values))
    codes = codes.reshape(bundles, features // bundles, codes.shape[1])
    codes = exchange(codes)
    return unpack(codes)


def solution(mesh):
    in_specs = (P(("rows", "bundle"), None), P(("rows", "bundle"), None), P(), P())
    out_specs = P("rows", "bundle")
    return jax.shard_map(local, mesh=mesh, in_specs=in_specs, out_specs=out_specs, check_vma=False)
```

```python
import functools

import jax
import jax.numpy as jnp
from jax import lax
from jax.experimental import pallas as pl
from jax.experimental.pallas import tpu as pltpu
from jax.sharding import PartitionSpec as P

LANES = 128
BLOCK = 128
MESH = pl.DeviceIdType.MESH


def lane_gather(table, index):
    return lax.gather(
        table,
        index[:, :, None],
        lax.GatherDimensionNumbers(
            offset_dims=(),
            collapsed_slice_dims=(1,),
            start_index_map=(1,),
            operand_batching_dims=(0,),
            start_indices_batching_dims=(0,),
        ),
        slice_sizes=(1, 1),
        mode=lax.GatherScatterMode.PROMISE_IN_BOUNDS,
    )


def table_kernel(edges_ref, table_ref):
    edges = edges_ref[...]
    tail = jnp.zeros((edges.shape[0], 2 * LANES - edges.shape[1]), jnp.float32)
    low = edges[:, :LANES]
    high = jnp.concatenate([edges[:, LANES:], tail], axis=1)
    lane = lax.broadcasted_iota(jnp.int32, low.shape, 1)
    for start in range(2):
        index = 2 * lane + 1 - start
        inner = index & (LANES - 1)
        picked = jnp.where(index < LANES, lane_gather(low, inner), lane_gather(high, inner))
        table_ref[:, start * LANES : (start + 1) * LANES] = picked


def make_tables(edges):
    count = edges.shape[0]
    return pl.pallas_call(
        table_kernel,
        out_shape=jax.ShapeDtypeStruct((count, 2 * LANES), jnp.float32),
        name="make_tables",
    )(edges)


def bin_codes_of(values, table):
    odd, even = table[:, :LANES], table[:, LANES:]
    middle = LANES // 2 - 1
    root = jnp.broadcast_to(odd[:, middle : middle + 1], odd.shape)
    halves = []
    for half in range(2):
        x = values[:, half * LANES : (half + 1) * LANES]
        step = LANES // 4
        at = jnp.where(x > root, middle + step, middle - step)
        while step > 1:
            step //= 2
            at = at + jnp.where(x > lane_gather(odd, at), step, -step)
        at = at + jnp.where(x > lane_gather(odd, at), 1, 0)
        halves.append(at + at + jnp.where(x > lane_gather(even, at), 1, 0))
    return halves[0] | (halves[1] << 16)


def bin_kernel(
    table_ref, raw_hbm, code_ref, all_ref, raw_ref, values_ref, raw_sem, send_sem, row_sem, side_sem, relay_sem, partner_sem
):
    held = table_ref.shape[0]
    rows, bundles = lax.axis_size("rows"), lax.axis_size("bundle")
    row, bundle = lax.axis_index("rows"), lax.axis_index("bundle")
    sides = bundles // 2
    flip = 1 - 2 * lax.rem(bundle, 2)
    partner = bundle + flip
    group = [lax.rem(row + step, rows) for step in range(rows)]
    origin = [lax.rem(row + rows - step, rows) for step in range(rows)]
    square = sides == 4
    if square:
        pair = lax.div(bundle, 2)
        across = bundle + 2 - 4 * lax.rem(pair, 2)
        along = bundle + 4 - 8 * lax.div(pair, 2)
        corner = across + 4 - 8 * lax.div(pair, 2)
        target = [bundle, across, along]
        source = [bundle, across, along, corner]
    else:
        target = [lax.rem(bundle + 2 * step, bundles) for step in range(sides)]
        source = [lax.rem(bundle + bundles - 2 * step, bundles) for step in range(sides)]
    near = len(target)

    fetch = pltpu.make_async_copy(raw_hbm, raw_ref, raw_sem)
    fetch.start()
    barrier = pltpu.get_barrier_semaphore()
    others = [(peer, bundle) for peer in group[1:]] + [(row, peer) for peer in target[1:]] + [(row, partner)]
    for peer in others:
        pl.semaphore_signal(barrier, inc=1, device_id=peer, device_id_type=MESH)
    pl.semaphore_wait(barrier, len(others))

    def place(row_index, bundle_index):
        return (row_index * bundles + bundle_index) * held

    def at(row_index, bundle_index, start=0, size=held):
        first = place(row_index, bundle_index) + start
        return all_ref.at[pl.ds(pl.multiple_of(first, 8), size)]

    sent = []

    def send(block, source_ref, device, arrival):
        copy = pltpu.make_async_remote_copy(
            src_ref=source_ref,
            dst_ref=block,
            send_sem=send_sem.at[len(sent)],
            recv_sem=arrival,
            device_id=device,
            device_id_type=MESH,
        )
        copy.start()
        sent.append(copy)

    def arrived(block, arrival):
        pltpu.make_async_copy(block, block, arrival).wait()

    def use(blocks):
        firsts = [place(*block) for block in blocks]

        def body(index, carry):
            first = firsts[0]
            for other in range(1, len(firsts)):
                first = jnp.where(index == other, firsts[other], first)
            span = pl.ds(pl.multiple_of(first, 8), held)
            code_ref[span, :] = bin_codes_of(values_ref[span, :], all_ref[span, :])
            return carry

        lax.fori_loop(0, len(firsts), body, 0)

    half = held // 2
    for step in range(1, rows):
        send(at(row, bundle), table_ref, (group[step], bundle), row_sem.at[step])
    for stage in range(rows + 3):
        ready = []
        if stage < rows:
            block = at(origin[stage], bundle)
            if stage:
                arrived(block, row_sem.at[stage])
            from_ref = block if stage else table_ref
            for turn in range(1, near):
                send(block, from_ref, (row, target[turn]), side_sem.at[stage, turn])
            send(block, from_ref, (row, partner), partner_sem.at[stage, 0])
            ready.append((origin[stage], bundle))
        if stage == 0:
            all_ref[pl.ds(pl.multiple_of(place(row, bundle), 8), held), :] = table_ref[...]
            fetch.wait()

            def turn_over(index, carry):
                span = pl.ds(pl.multiple_of(index * LANES, LANES), LANES)
                values_ref[span, :] = raw_ref[:, span].T
                return carry

            lax.fori_loop(0, raw_ref.shape[1] // LANES, turn_over, 0)
        step = stage - 1
        if 0 <= step < rows:
            for turn in range(1, near):
                block = at(origin[step], source[turn])
                arrived(block, side_sem.at[step, turn])
                if square:
                    start = half * (2 - turn)
                    part = at(origin[step], source[turn], start, half)
                    send(part, part, (row, target[3 - turn]), relay_sem.at[step, 2 - turn])
                send(block, block, (row, partner), partner_sem.at[step, turn])
                ready.append((origin[step], source[turn]))
            arrived(at(origin[step], partner), partner_sem.at[step, 0])
            ready.append((origin[step], partner))
        step = stage - 2
        if 0 <= step < rows:
            if square:
                arrived(at(origin[step], corner, 0, half), relay_sem.at[step, 0])
                arrived(at(origin[step], corner, half, half), relay_sem.at[step, 1])
                block = at(origin[step], corner)
                send(block, block, (row, partner), partner_sem.at[step, 3])
                ready.append((origin[step], corner))
            for turn in range(1, near):
                arrived(at(origin[step], source[turn] + flip), partner_sem.at[step, turn])
                ready.append((origin[step], source[turn] + flip))
        step = stage - 3
        if 0 <= step < rows and square:
            arrived(at(origin[step], corner + flip), partner_sem.at[step, 3])
            ready.append((origin[step], corner + flip))
        if ready:
            use(ready)
    for copy in sent:
        copy.wait_send()


def bin_rows(tables, raw):
    held, width = tables.shape
    count, features = raw.shape
    rows, bundles = lax.axis_size("rows"), lax.axis_size("bundle")
    sides = bundles // 2
    sends = rows - 1 + rows * 3 * sides
    return pl.pallas_call(
        bin_kernel,
        out_shape=jax.ShapeDtypeStruct((features, count // 2), jnp.int32),
        in_specs=[pl.BlockSpec(memory_space=pltpu.VMEM), pl.BlockSpec(memory_space=pl.ANY)],
        out_specs=pl.BlockSpec(memory_space=pltpu.VMEM),
        scratch_shapes=[
            pltpu.VMEM((features, width), jnp.float32),
            pltpu.VMEM((count, features), jnp.float32),
            pltpu.VMEM((features, count), jnp.float32),
            pltpu.SemaphoreType.DMA,
            pltpu.SemaphoreType.DMA((sends,)),
            pltpu.SemaphoreType.DMA((rows,)),
            pltpu.SemaphoreType.DMA((rows, sides)),
            pltpu.SemaphoreType.DMA((rows, 2)),
            pltpu.SemaphoreType.DMA((rows, sides)),
        ],
        compiler_params=pltpu.CompilerParams(collective_id=0, has_side_effects=True),
        name="bin_rows",
    )(tables, raw)


def order_kernel(column_ref, offset_ref, code_ref, out_ref):
    def body(index, carry):
        first = pl.multiple_of(index * BLOCK, BLOCK)
        offset = jnp.broadcast_to(offset_ref[pl.ds(index, 1), :], (BLOCK, BLOCK)).T[:, : code_ref.shape[1]]
        codes = code_ref[pl.ds(first, BLOCK), :] + (offset | (offset << 16))
        for row in range(BLOCK):
            out_ref[pl.ds(column_ref[first + row], 1), :] = codes[row : row + 1, :]
        return carry

    lax.fori_loop(0, code_ref.shape[0] // BLOCK, body, 0)


def order_columns(column, offset, codes):
    return pl.pallas_call(
        order_kernel,
        out_shape=jax.ShapeDtypeStruct(codes.shape, jnp.int32),
        in_specs=[
            pl.BlockSpec(memory_space=pltpu.SMEM),
            pl.BlockSpec(memory_space=pltpu.VMEM),
            pl.BlockSpec(memory_space=pltpu.VMEM),
        ],
        out_specs=pl.BlockSpec(memory_space=pltpu.VMEM),
        name="order_columns",
    )(column, offset.reshape(-1, BLOCK), codes)


def exchange_kernel(code_ref, out_ref, own_ref, own_sem, send_sem, arrive_sem):
    bundles = lax.axis_size("bundle")
    row, bundle = lax.axis_index("rows"), lax.axis_index("bundle")
    keep = pltpu.make_async_copy(code_ref.at[bundle], own_ref, own_sem)
    keep.start()
    barrier = pltpu.get_barrier_semaphore()
    peers = [lax.rem(bundle + step, bundles) for step in range(bundles)]
    for peer in peers[1:]:
        pl.semaphore_signal(barrier, inc=1, device_id=(row, peer), device_id_type=MESH)
    pl.semaphore_wait(barrier, bundles - 1)
    sent = []
    for step in range(1, bundles):
        copy = pltpu.make_async_remote_copy(
            src_ref=code_ref.at[peers[step]],
            dst_ref=out_ref.at[bundle],
            send_sem=send_sem.at[step],
            recv_sem=arrive_sem.at[step],
            device_id=(row, peers[step]),
            device_id_type=MESH,
        )
        copy.start()
        sent.append(copy)
    keep.wait()
    keep = pltpu.make_async_copy(own_ref, out_ref.at[bundle], own_sem)
    keep.start()
    for step in range(1, bundles):
        block = out_ref.at[lax.rem(bundle + bundles - step, bundles)]
        pltpu.make_async_copy(block, block, arrive_sem.at[step]).wait()
    for copy in sent:
        copy.wait_send()
    keep.wait()


def exchange(codes):
    bundles, columns, width = codes.shape
    return pl.pallas_call(
        exchange_kernel,
        out_shape=jax.ShapeDtypeStruct(codes.shape, jnp.int32),
        in_specs=[pl.BlockSpec(memory_space=pl.ANY)],
        out_specs=pl.BlockSpec(memory_space=pl.ANY),
        scratch_shapes=[
            pltpu.VMEM((columns, width), jnp.int32),
            pltpu.SemaphoreType.DMA,
            pltpu.SemaphoreType.DMA((bundles,)),
            pltpu.SemaphoreType.DMA((bundles,)),
        ],
        compiler_params=pltpu.CompilerParams(collective_id=1, has_side_effects=True),
        name="exchange",
    )(codes)


def unpack_kernel(code_ref, out_ref):
    sources, _, half = code_ref.shape
    for source in range(sources):
        codes = code_ref[source].T
        start = 2 * half * source
        out_ref[start : start + half, :] = codes & 65535
        out_ref[start + half : start + 2 * half, :] = codes >> 16


def unpack(codes):
    sources, columns, half = codes.shape
    block = 2
    return pl.pallas_call(
        unpack_kernel,
        grid=(sources // block,),
        in_specs=[pl.BlockSpec((block, columns, half), lambda i: (i, 0, 0))],
        out_specs=pl.BlockSpec((block * 2 * half, columns), lambda i: (i, 0)),
        out_shape=jax.ShapeDtypeStruct((sources * 2 * half, columns), jnp.int32),
        name="unpack",
    )(codes)


def local(raw_values, bin_edges, feature_column, bin_offset):
    bundles = lax.axis_size("bundle")
    features = feature_column.shape[0]
    codes = bin_rows(make_tables(bin_edges), raw_values)
    codes = order_columns(feature_column, bin_offset, codes)
    codes = codes.reshape(bundles, features // bundles, codes.shape[1])
    codes = exchange(codes)
    return unpack(codes)


def solution(mesh):
    in_specs = (P(("rows", "bundle"), None), P(("rows", "bundle"), None), P(), P())
    out_specs = P("rows", "bundle")
    return jax.shard_map(local, mesh=mesh, in_specs=in_specs, out_specs=out_specs, check_vma=False)
```
